256 devices in a mesh: vel: 32 (over z, x_lo, core), gx: 8 (over y, x_hi).
Axes of the slice: x: 4 (x_hi: 2, x_lo: 2; x = x_hi * 2 + x_lo), y: 4, z: 8, core: 2. Of those that a mesh axis runs over, the one named last changes fastest.
Arguments:
- distribution: float32 [4096, 32, 256], P('vel', 'gx'), as said below
Outputs:
- relaxed: float32 [4096, 32, 256], P('vel', 'gx')
Inputs may be any that keep to these rules, and one draw needn't show every extreme that they name: `distribution`: every entry is positive.
All inputs are finite; a program needn't handle non-finite values.
Results may differ from the reference program's by a relative error of at most 0.0003.
Values sent between devices are 32-bit elements; how exact they have to be, the bound alone decides.
No kernel may reach another device: no remote copies, remote signals or barrier semaphores. Data moves between devices by JAX's collectives and lax.ppermute only.
A program may use at most 64 MiB of HBM per device.

```python
import math
import jax
import jax.numpy as jnp
from jax import lax

NV1 = 16
V = 4096
NY = 16
NZ = 16
COLLISIONS = 2
NX = 32


def draw_distribution(key, part):
    keys = jax.random.split(jax.random.fold_in(key, 17), 4)
    cells = NX * NY * NZ
    rho = jnp.exp(jax.random.uniform(keys[0], (cells,), jnp.float32, math.log(0.5), math.log(2.0)))
    drift = jax.random.uniform(keys[1], (3, cells), jnp.float32, -1.0, 1.0)
    temp = jnp.exp(jax.random.uniform(keys[2], (cells,), jnp.float32, math.log(0.6), math.log(2.5)))
    rough = 0.4 * jax.random.uniform(keys[3], (V, cells), jnp.float32, -1.0, 1.0)
    spacing = 8.0 / (NV1 - 1)
    index = jnp.arange(V, dtype=jnp.int32)
    first = (-4.0 + spacing * (index % NV1).astype(jnp.float32))[:, None]
    second = (-4.0 + spacing * (index // NV1 // NV1).astype(jnp.float32))[:, None]
    third = (-4.0 + spacing * (index // NV1 % NV1).astype(jnp.float32))[:, None]
    spread = (first - drift[0]) ** 2 + (second - drift[1]) ** 2 + (third - drift[2]) ** 2
    field = rho * temp ** (-1.5) * jnp.exp(-spread / (2.0 * temp)) * (1.0 + rough)
    return field.reshape(V, NX, NY * NZ).astype(jnp.float32)


def setup_inputs(seed: int = 0) -> dict:
    key_of = jax.random.split(jax.random.key(seed), 2)
    distribution = draw_distribution(jax.random.fold_in(key_of[1], 71), 0)
    return {"distribution": distribution}


speed_limit = 4.0
time_step = 0.05
knudsen = 0.0125
vel_block = 256

def velocities(index):
    spacing = 2.0 * speed_limit / (NV1 - 1)
    first = index % NV1
    rest = index // NV1
    second = rest // NV1
    third = rest % NV1
    return [-speed_limit + spacing * part.astype(jnp.float32) for part in (first, second, third)]

def quad_weight():
    spacing = 2.0 * speed_limit / (NV1 - 1)
    return spacing ** 3 / (2.0 * math.pi) ** 1.5

def along_z(field, offset):
    zpos = jnp.arange(field.shape[-1], dtype=jnp.int32) % NZ
    main = jnp.roll(field, offset, -1)
    if offset > 0:
        other = jnp.roll(field, offset - NZ, -1)
        keep = zpos >= offset
    else:
        other = jnp.roll(field, offset + NZ, -1)
        keep = zpos < NZ + offset
    return jnp.where(keep, main, other)

def backward(field, minus_one, minus_two):
    return (3.0 * field - 4.0 * minus_one + minus_two) * 0.5

def forward(field, plus_one, plus_two):
    return (-3.0 * field + 4.0 * plus_one - plus_two) * 0.5

def upwind(field, comp, minus_one, minus_two, plus_one, plus_two):
    return jnp.where(comp > 0, backward(field, minus_one, minus_two), forward(field, plus_one, plus_two))

def transverse(field, comp_y, comp_z):
    deriv_y = upwind(field, comp_y, jnp.roll(field, NZ, -1), jnp.roll(field, 2 * NZ, -1), jnp.roll(field, -NZ, -1), jnp.roll(field, -2 * NZ, -1))
    deriv_z = upwind(field, comp_z, along_z(field, 1), along_z(field, 2), along_z(field, -1), along_z(field, -2))
    return (deriv_y, deriv_z)

def rate(field, comp_x, comp_y, comp_z):
    deriv_x = upwind(field, comp_x, jnp.roll(field, 1, 1), jnp.roll(field, 2, 1), jnp.roll(field, -1, 1), jnp.roll(field, -2, 1))
    deriv_y, deriv_z = transverse(field, comp_y, comp_z)
    return -(comp_x * deriv_x + comp_y * deriv_y + comp_z * deriv_z)

def advance(field, comp_x, comp_y, comp_z):
    first = field + time_step * rate(field, comp_x, comp_y, comp_z)
    second = 0.75 * field + 0.25 * (first + time_step * rate(first, comp_x, comp_y, comp_z))
    return field / 3.0 + 2.0 / 3.0 * (second + time_step * rate(second, comp_x, comp_y, comp_z))

def primitive(moments):
    rho = moments[0]
    vel_x = moments[1] / rho
    vel_y = moments[2] / rho
    vel_z = moments[3] / rho
    temp = (moments[4] / rho - (vel_x * vel_x + vel_y * vel_y + vel_z * vel_z)) / 3.0
    return jnp.stack([rho, vel_x, vel_y, vel_z, temp])

def maxwell(prims, comp_x, comp_y, comp_z):
    spread = (comp_x - prims[1]) ** 2 + (comp_y - prims[2]) ** 2 + (comp_z - prims[3]) ** 2
    return prims[0] * prims[4] ** (-1.5) * jnp.exp(-spread / (2.0 * prims[4]))

def moment_table(comp_x, comp_y, comp_z):
    ones = jnp.ones_like(comp_x)
    return jnp.stack([ones, comp_x, comp_y, comp_z, comp_x * comp_x + comp_y * comp_y + comp_z * comp_z]) * quad_weight()

def reference(distribution):
    blocks = V // vel_block
    index = jnp.arange(V, dtype=jnp.int32)
    comp = jnp.stack(velocities(index), 1).reshape(blocks, vel_block, 3)
    field = distribution.reshape(blocks, vel_block, NX, NY * NZ)

    def stream(args):
        block, cv = args
        return advance(block, cv[:, 0][:, None, None], cv[:, 1][:, None, None], cv[:, 2][:, None, None])
    for step in range(COLLISIONS):
        field = lax.map(stream, (field, comp))

        def moment_block(args):
            block, cv = args
            table = moment_table(cv[:, 0], cv[:, 1], cv[:, 2])
            return jnp.dot(table, block.reshape(vel_block, -1), precision=lax.Precision.HIGHEST)
        moments = lax.optimization_barrier(jnp.sum(lax.map(moment_block, (field, comp)), 0))
        prims = primitive(moments)

        def mass_block(cv):
            local = maxwell(prims, cv[:, 0][:, None], cv[:, 1][:, None], cv[:, 2][:, None])
            return quad_weight() * lax.optimization_barrier(jnp.sum(local, 0))
        mass = lax.optimization_barrier(jnp.sum(lax.map(mass_block, comp), 0))
        scale = prims[0] / mass
        rates = time_step * prims[0] * jnp.sqrt(prims[4]) / knudsen

        def relax(args):
            block, cv = args
            local = maxwell(prims, cv[:, 0][:, None], cv[:, 1][:, None], cv[:, 2][:, None])
            flat = block.reshape(vel_block, -1)
            return ((flat + rates * (local * scale)) / (1.0 + rates)).reshape(block.shape)
        field = lax.map(relax, (field, comp))
    return field.reshape(V, NX, NY * NZ)
```

```python
import math

import jax
import jax.numpy as jnp
from jax import lax
from jax.experimental import pallas as pl
from jax.experimental.pallas import tpu as pltpu
from jax.sharding import PartitionSpec as P

NV1 = 16
COLLISIONS = 2

speed_limit = 4.0
time_step = 0.05
knudsen = 0.0125
spacing = 2.0 * speed_limit / (NV1 - 1)
weight = spacing**3 / (2.0 * math.pi) ** 1.5

PLANES = 4
CZ = 8
CX = 8
LANES = 128
YZ = 256


def point(index):
    return -speed_limit + spacing * index.astype(jnp.float32)


def cx_column(half):
    return point(half * CX + lax.broadcasted_iota(jnp.int32, (CX, LANES), 0))


def stream_kernel(vel_ref, up0, up1, up2, down0, down1, down2, up_out, down_out, mom_out):
    vel = vel_ref[0]
    iy = vel // 2
    zhalf = vel % 2
    cy = point(iy)
    ay = time_step * jnp.abs(cy)
    ypos = iy >= NV1 // 2
    zpos = zhalf == 1
    lane = lax.broadcasted_iota(jnp.int32, (CX, LANES), 1)
    zlane = lane % 16
    ylane = jnp.where(ypos, lane, LANES - 1 - lane)
    zlane = jnp.where(zpos, zlane, 15 - zlane)
    masks_y = (ylane < 16, ylane < 32)
    masks_z = (zlane < 1, zlane < 2)
    rolls_y = (jnp.where(ypos, 16, 112), jnp.where(ypos, 32, 96))
    rolls_z = (jnp.where(zpos, 1, 127), jnp.where(zpos, 2, 126))
    wraps_z = (jnp.where(zpos, 113, 15), jnp.where(zpos, 114, 14))

    def shift_y(pair, by):
        rolled = [pltpu.roll(part, rolls_y[by], 1) for part in pair]
        mask = masks_y[by]
        return (jnp.where(mask, rolled[1], rolled[0]), jnp.where(mask, rolled[0], rolled[1]))

    def shift_z(part, by):
        return jnp.where(
            masks_z[by], pltpu.roll(part, wraps_z[by], 1), pltpu.roll(part, rolls_z[by], 1)
        )

    def block(iz, _):
        cz = point(zhalf * CZ + iz)
        az = time_step * jnp.abs(cz)
        for half in (0, 1):
            ax = time_step * jnp.abs(cx_column(half))
            keep = 1.0 - 1.5 * (ax + (ay + az))

            def section(now, one, two):
                y1, y2 = shift_y(now, 0), shift_y(now, 1)
                out = []
                for t in (0, 1):
                    along_x = (2.0 * ax) * one[t] - (0.5 * ax) * two[t]
                    along_y = (2.0 * ay) * y1[t] - (0.5 * ay) * y2[t]
                    along_z = (2.0 * az) * shift_z(now[t], 0) - (0.5 * az) * shift_z(now[t], 1)
                    out.append(keep * now[t] + (along_x + (along_y + along_z)))
                return out

            if half:
                planes = [(up2, 0), (up2, 1)] + [(up1, p) for p in range(PLANES)]
                planes += [(up0, p) for p in range(PLANES)]
            else:
                planes = [(down2, 1), (down2, 0)] + [(down1, p) for p in reversed(range(PLANES))]
                planes += [(down0, p) for p in reversed(range(PLANES))]
            sixth, first, second = {}, {}, {}
            for p, (ref, plane) in enumerate(planes):
                sixth[p] = [
                    ref[plane, iz, :, t * LANES : (t + 1) * LANES] * (1.0 / 6.0) for t in (0, 1)
                ]
                if p >= 2:
                    first[p] = section(sixth[p], sixth[p - 1], sixth[p - 2])
                if p >= 4:
                    moved = section(first[p], first[p - 1], first[p - 2])
                    second[p] = [3.0 * a + b for a, b in zip(sixth[p], moved)]
                if p >= 6:
                    moved = section(second[p], second[p - 1], second[p - 2])
                    out = up_out if half else down_out
                    for t in (0, 1):
                        out[plane, iz, :, t * LANES : (t + 1) * LANES] = (
                            2.0 * sixth[p][t] + moved[t]
                        )
        return 0

    lax.fori_loop(0, CZ, block, 0)

    for plane in range(PLANES):
        for t in (0, 1):
            cols = slice(t * LANES, (t + 1) * LANES)
            total = [0.0] * 5
            for half, out in ((0, down_out), (1, up_out)):
                zero = jnp.zeros((CX, LANES), jnp.float32)
                plain, lin, quad = zero, zero, zero
                for iz in range(CZ):
                    cz = point(zhalf * CZ + iz)
                    read = out[plane, iz, :, cols]
                    plain += read
                    lin += cz * read
                    quad += (cz * cz) * read
                cx = cx_column(half)
                terms = (plain, cx * plain, cy * plain, lin, (cx * cx + cy * cy) * plain + quad)
                total = [a + b for a, b in zip(total, terms)]
            for which in range(5):
                row = plane * 2 + t
                mom_out[which, row : row + 1, :] = weight * jnp.sum(
                    total[which], axis=0, keepdims=True
                )


def relax_kernel(last, vel_ref, mom_ref, up_in, down_in, *outs_and_scratch):
    *outs, rows = outs_and_scratch
    vel = vel_ref[0]
    cy = point(vel // 2)
    zhalf = vel % 2
    rho = mom_ref[0]
    ux = mom_ref[1] / rho
    uy = mom_ref[2] / rho
    uz = mom_ref[3] / rho
    temp = (mom_ref[4] / rho - (ux * ux + uy * uy + uz * uz)) / 3.0
    minus_half = -0.5 / temp

    def factor(c, u, scale):
        return jnp.exp((c - u) * (c - u) * scale)

    def total(u):
        out = jnp.zeros_like(u)
        for i in range(NV1):
            out += factor(-speed_limit + spacing * i, u, minus_half)
        return out

    root = jnp.sqrt(temp)
    peak = rho / (temp * root)
    mass = weight * peak * total(ux) * total(uy) * total(uz)
    nu = time_step * rho * root / knudsen
    shrink = 1.0 / (1.0 + nu)
    common = nu * shrink * peak * (rho / mass) * factor(cy, uy, minus_half)
    for iz in range(CZ):
        rows[iz] = common * factor(point(zhalf * CZ + iz), uz, minus_half)
    rows[CZ] = shrink
    rows[CZ + 1] = ux
    rows[CZ + 2] = minus_half

    def row(which, index):
        return jnp.broadcast_to(rows[which, index : index + 1, :], (CX, LANES))

    for plane in range(PLANES):
        for t in (0, 1):
            cols = slice(t * LANES, (t + 1) * LANES)
            index = plane * 2 + t
            keep, drift, scale = (row(CZ + k, index) for k in range(3))
            both = [factor(cx_column(half), drift, scale) for half in (0, 1)]
            for iz in range(CZ):
                gain = row(iz, index)
                for half, ref in ((0, down_in), (1, up_in)):
                    value = ref[plane, iz, :, cols] * keep + both[half] * gain
                    if last:
                        outs[0][plane, iz, half, :, cols] = value
                    else:
                        outs[half][plane, iz, :, cols] = value
                        if half == 0 and plane < 2:
                            outs[2][plane, iz, :, cols] = value
                        if half == 1 and plane >= 2:
                            outs[3][plane - 2, iz, :, cols] = value


def vmem():
    return pl.BlockSpec(memory_space=pltpu.VMEM)


def smem():
    return pl.BlockSpec(memory_space=pltpu.SMEM)


def shape(*sizes):
    return jax.ShapeDtypeStruct(sizes, jnp.float32)


def stream(vel, up, down):
    return pl.pallas_call(
        stream_kernel,
        in_specs=[smem()] + [vmem()] * 6,
        out_specs=[vmem()] * 3,
        out_shape=[
            shape(PLANES, CZ, CX, YZ),
            shape(PLANES, CZ, CX, YZ),
            shape(5, 2 * PLANES, LANES),
        ],
        name="stream",
    )(vel, *up, *down)


def relax(vel, moments, up, down, last):
    if last:
        out_shape = [shape(PLANES, CZ, 2, CX, YZ)]
    else:
        out_shape = [shape(PLANES, CZ, CX, YZ)] * 2 + [shape(2, CZ, CX, YZ)] * 2

    def body(*refs):
        relax_kernel(last, *refs)

    return pl.pallas_call(
        body,
        in_specs=[smem()] + [vmem()] * 3,
        out_specs=[vmem()] * len(out_shape),
        out_shape=out_shape,
        scratch_shapes=[pltpu.VMEM((CZ + 3, 2 * PLANES, LANES), jnp.float32)],
        name="relax_last" if last else "relax",
    )(vel, moments, up, down)


def passed_along(value, by):
    size = lax.axis_size("gx")
    return lax.ppermute(value, "gx", [(i, (i + by) % size) for i in range(size)])


def summed_over_velocities(value):
    size = lax.axis_size("vel")
    bit = 1
    while bit < size:
        value = value + lax.ppermute(value, "vel", [(i, i ^ bit) for i in range(size)])
        bit *= 2
    return value


def on_device(distribution):
    vel = lax.axis_index("vel").astype(jnp.int32).reshape(1)
    field = distribution.reshape(CZ, 2, CX, PLANES, YZ)
    up = field[:, 1].transpose(2, 0, 1, 3)
    down = field[:, 0].transpose(2, 0, 1, 3)
    up_far, down_far = up[2:], down[:2]
    for step in range(COLLISIONS):
        ups = (up, passed_along(up, 1), passed_along(up_far, 2))
        downs = (down, passed_along(down, -1), passed_along(down_far, -2))
        up_read, down_read, moments = stream(vel, ups, downs)
        moments = summed_over_velocities(moments)
        outs = relax(vel, moments, up_read, down_read, step == COLLISIONS - 1)
        if step < COLLISIONS - 1:
            down, up, down_far, up_far = outs
    return outs[0].transpose(1, 2, 3, 0, 4).reshape(distribution.shape)


def solution(mesh):
    return jax.shard_map(
        on_device,
        mesh=mesh,
        in_specs=(P("vel", "gx", None),),
        out_specs=P("vel", "gx", None),
        check_vma=False,
    )
```

```python
import math

import jax
import jax.numpy as jnp
from jax import lax
from jax.experimental import pallas as pl
from jax.experimental.pallas import tpu as pltpu
from jax.sharding import PartitionSpec as P

NV1 = 16
COLLISIONS = 2

speed_limit = 4.0
time_step = 0.05
knudsen = 0.0125
spacing = 2.0 * speed_limit / (NV1 - 1)
weight = spacing**3 / (2.0 * math.pi) ** 1.5

PLANES = 4
CZ = 8
CX = 8
LANES = 128
YZ = 256


def point(index):
    return -speed_limit + spacing * index.astype(jnp.float32)


def cx_column(half):
    return point(half * CX + lax.broadcasted_iota(jnp.int32, (CX, LANES), 0))


def stream_kernel(vel_ref, up0, up1, up2, down0, down1, down2, up_out, down_out, mom_out):
    vel = vel_ref[0]
    iy = vel // 2
    zhalf = vel % 2
    cy = point(iy)
    ay = time_step * jnp.abs(cy)
    ypos = iy >= NV1 // 2
    zpos = zhalf == 1
    lane = lax.broadcasted_iota(jnp.int32, (CX, LANES), 1)
    zlane = lane % 16
    ylane = jnp.where(ypos, lane, LANES - 1 - lane)
    zlane = jnp.where(zpos, zlane, 15 - zlane)
    masks_y = (ylane < 16, ylane < 32)
    masks_z = (zlane < 1, zlane < 2)
    rolls_y = (jnp.where(ypos, 16, 112), jnp.where(ypos, 32, 96))
    rolls_z = (jnp.where(zpos, 1, 127), jnp.where(zpos, 2, 126))
    wraps_z = (jnp.where(zpos, 113, 15), jnp.where(zpos, 114, 14))

    def shift_y(pair, by):
        rolled = [pltpu.roll(part, rolls_y[by], 1) for part in pair]
        mask = masks_y[by]
        return (jnp.where(mask, rolled[1], rolled[0]), jnp.where(mask, rolled[0], rolled[1]))

    def shift_z(part, by):
        return jnp.where(
            masks_z[by], pltpu.roll(part, wraps_z[by], 1), pltpu.roll(part, rolls_z[by], 1)
        )

    def block(iz, _):
        cz = point(zhalf * CZ + iz)
        az = time_step * jnp.abs(cz)
        for half in (0, 1):
            ax = time_step * jnp.abs(cx_column(half))
            keep = 1.0 - 1.5 * (ax + (ay + az))

            def section(now, one, two):
                y1, y2 = shift_y(now, 0), shift_y(now, 1)
                out = []
                for t in (0, 1):
                    along_x = (2.0 * ax) * one[t] - (0.5 * ax) * two[t]
                    along_y = (2.0 * ay) * y1[t] - (0.5 * ay) * y2[t]
                    along_z = (2.0 * az) * shift_z(now[t], 0) - (0.5 * az) * shift_z(now[t], 1)
                    out.append(keep * now[t] + (along_x + (along_y + along_z)))
                return out

            if half:
                planes = [(up2, 0), (up2, 1)] + [(up1, p) for p in range(PLANES)]
                planes += [(up0, p) for p in range(PLANES)]
            else:
                planes = [(down2, 1), (down2, 0)] + [(down1, p) for p in reversed(range(PLANES))]
                planes += [(down0, p) for p in reversed(range(PLANES))]
            sixth, first, second = {}, {}, {}
            for p, (ref, plane) in enumerate(planes):
                sixth[p] = [
                    ref[plane, iz, :, t * LANES : (t + 1) * LANES] * (1.0 / 6.0) for t in (0, 1)
                ]
                if p >= 2:
                    first[p] = section(sixth[p], sixth[p - 1], sixth[p - 2])
                if p >= 4:
                    moved = section(first[p], first[p - 1], first[p - 2])
                    second[p] = [3.0 * a + b for a, b in zip(sixth[p], moved)]
                if p >= 6:
                    moved = section(second[p], second[p - 1], second[p - 2])
                    out = up_out if half else down_out
                    for t in (0, 1):
                        out[plane, iz, :, t * LANES : (t + 1) * LANES] = (
                            2.0 * sixth[p][t] + moved[t]
                        )
        return 0

    lax.fori_loop(0, CZ, block, 0)

    for plane in range(PLANES):
        for t in (0, 1):
            cols = slice(t * LANES, (t + 1) * LANES)
            total = [0.0] * 5
            for half, out in ((0, down_out), (1, up_out)):
                zero = jnp.zeros((CX, LANES), jnp.float32)
                plain, lin, quad = zero, zero, zero
                for iz in range(CZ):
                    cz = point(zhalf * CZ + iz)
                    read = out[plane, iz, :, cols]
                    plain += read
                    lin += cz * read
                    quad += (cz * cz) * read
                cx = cx_column(half)
                terms = (plain, cx * plain, cy * plain, lin, (cx * cx + cy * cy) * plain + quad)
                total = [a + b for a, b in zip(total, terms)]
            for which in range(5):
                row = plane * 2 + t
                mom_out[which, row : row + 1, :] = weight * jnp.sum(
                    total[which], axis=0, keepdims=True
                )


def relax_kernel(last, vel_ref, mom_ref, up_in, down_in, *outs_and_scratch):
    *outs, rows = outs_and_scratch
    vel = vel_ref[0]
    cy = point(vel // 2)
    zhalf = vel % 2
    rho = mom_ref[0]
    ux = mom_ref[1] / rho
    uy = mom_ref[2] / rho
    uz = mom_ref[3] / rho
    temp = (mom_ref[4] / rho - (ux * ux + uy * uy + uz * uz)) / 3.0
    minus_half = -0.5 / temp

    def factor(c, u, scale):
        return jnp.exp((c - u) * (c - u) * scale)

    def total(u):
        out = jnp.zeros_like(u)
        for i in range(NV1):
            out += factor(-speed_limit + spacing * i, u, minus_half)
        return out

    root = jnp.sqrt(temp)
    peak = rho / (temp * root)
    mass = weight * peak * total(ux) * total(uy) * total(uz)
    nu = time_step * rho * root / knudsen
    shrink = 1.0 / (1.0 + nu)
    common = nu * shrink * peak * (rho / mass) * factor(cy, uy, minus_half)
    for iz in range(CZ):
        rows[iz] = common * factor(point(zhalf * CZ + iz), uz, minus_half)
    rows[CZ] = shrink
    rows[CZ + 1] = ux
    rows[CZ + 2] = minus_half

    def row(which, index):
        return jnp.broadcast_to(rows[which, index : index + 1, :], (CX, LANES))

    for plane in range(PLANES):
        for t in (0, 1):
            cols = slice(t * LANES, (t + 1) * LANES)
            index = plane * 2 + t
            keep, drift, scale = (row(CZ + k, index) for k in range(3))
            both = [factor(cx_column(half), drift, scale) for half in (0, 1)]
            for iz in range(CZ):
                gain = row(iz, index)
                for half, ref in ((0, down_in), (1, up_in)):
                    value = ref[plane, iz, :, cols] * keep + both[half] * gain
                    if last:
                        outs[0][plane, iz, half, :, cols] = value
                    else:
                        outs[half][plane, iz, :, cols] = value
                        if half == 0 and plane < 2:
                            outs[2][plane, iz, :, cols] = value
                        if half == 1 and plane >= 2:
                            outs[3][plane - 2, iz, :, cols] = value


def vmem():
    return pl.BlockSpec(memory_space=pltpu.VMEM)


def smem():
    return pl.BlockSpec(memory_space=pltpu.SMEM)


def shape(*sizes):
    return jax.ShapeDtypeStruct(sizes, jnp.float32)


def stream(vel, up, down):
    return pl.pallas_call(
        stream_kernel,
        in_specs=[smem()] + [vmem()] * 6,
        out_specs=[vmem()] * 3,
        out_shape=[
            shape(PLANES, CZ, CX, YZ),
            shape(PLANES, CZ, CX, YZ),
            shape(5, 2 * PLANES, LANES),
        ],
        name="stream",
        compiler_params=pltpu.CompilerParams(vmem_limit_bytes=8 << 20),
    )(vel, *up, *down)


def relax(vel, moments, up, down, last):
    if last:
        out_shape = [shape(PLANES, CZ, 2, CX, YZ)]
    else:
        out_shape = [shape(PLANES, CZ, CX, YZ)] * 2 + [shape(2, CZ, CX, YZ)] * 2

    def body(*refs):
        relax_kernel(last, *refs)

    return pl.pallas_call(
        body,
        in_specs=[smem()] + [vmem()] * 3,
        out_specs=[vmem()] * len(out_shape),
        out_shape=out_shape,
        scratch_shapes=[pltpu.VMEM((CZ + 3, 2 * PLANES, LANES), jnp.float32)],
        name="relax_last" if last else "relax",
        compiler_params=pltpu.CompilerParams(vmem_limit_bytes=8 << 20),
    )(vel, moments, up, down)


def passed_along(value, by):
    size = lax.axis_size("gx")
    return lax.ppermute(value, "gx", [(i, (i + by) % size) for i in range(size)])


def summed_over_velocities(value):
    size = lax.axis_size("vel")
    bit = 1
    while bit < size:
        value = value + lax.ppermute(value, "vel", [(i, i ^ bit) for i in range(size)])
        bit *= 2
    return value


def on_device(distribution):
    vel = lax.axis_index("vel").astype(jnp.int32).reshape(1)
    field = distribution.reshape(CZ, 2, CX, PLANES, YZ)
    up = field[:, 1].transpose(2, 0, 1, 3)
    down = field[:, 0].transpose(2, 0, 1, 3)
    up_far, down_far = up[2:], down[:2]
    for step in range(COLLISIONS):
        ups = (up, passed_along(up, 1), passed_along(up_far, 2))
        downs = (down, passed_along(down, -1), passed_along(down_far, -2))
        up_read, down_read, moments = stream(vel, ups, downs)
        moments = summed_over_velocities(moments)
        outs = relax(vel, moments, up_read, down_read, step == COLLISIONS - 1)
        if step < COLLISIONS - 1:
            down, up, down_far, up_far = outs
    return outs[0].transpose(1, 2, 3, 0, 4).reshape(distribution.shape)


def solution(mesh):
    return jax.shard_map(
        on_device,
        mesh=mesh,
        in_specs=(P("vel", "gx", None),),
        out_specs=P("vel", "gx", None),
        check_vma=False,
    )
```

```python
import math

import jax
import jax.numpy as jnp
from jax import lax
from jax.experimental import pallas as pl
from jax.experimental.pallas import tpu as pltpu
from jax.sharding import PartitionSpec as P

NV1 = 16
COLLISIONS = 2

speed_limit = 4.0
time_step = 0.05
knudsen = 0.0125
spacing = 2.0 * speed_limit / (NV1 - 1)
weight = spacing**3 / (2.0 * math.pi) ** 1.5

PLANES = 4
NY = 16
CZ = 8
CX = 8
COUNT = 2 * CX * CZ
LANES = 128
TILE = (8, LANES)
ROWS = PLANES * NY
SPLIT = (PLANES, 2, COUNT, LANES)


def point(index):
    return -speed_limit + spacing * index.astype(jnp.float32)


def iota(dim):
    return lax.broadcasted_iota(jnp.int32, TILE, dim)


def cx_lanes(half):
    return point(half * CX + iota(1) % 8)


class Device:
    def __init__(self, vel):
        zhalf = vel % 2
        self.ypos = vel // 2 >= NV1 // 2
        self.zpos = zhalf == 1
        self.cy = point(vel // 2)
        self.cz = point(zhalf * CZ + iota(0))

    def row(self, plane, y):
        return plane * NY + jnp.where(self.ypos, y, NY - 1 - y)

    def base(self, yhalf):
        return jnp.where(self.ypos, yhalf, 1 - yhalf) * 8

    def mirror_z(self, tile):
        lane = iota(1)
        source = jnp.where(self.zpos, lane, (15 - lane // 8) * 8 + lane % 8)
        return permuted(tile, source)


def permuted(tile, source):
    return jnp.take_along_axis(tile, source, axis=1, mode="promise_in_bounds")


def swapped(tiles):
    tiles = list(tiles)
    lane = iota(1)
    for w in (1, 2, 4):
        high = (lane // w) % 2 == 1
        for i in range(8):
            if not i & w:
                a, b = tiles[i], tiles[i + w]
                tiles[i] = jnp.where(high, pltpu.roll(b, w, 1), a)
                tiles[i + w] = jnp.where(high, b, pltpu.roll(a, LANES - w, 1))
    return tiles


def pack_kernel(vel_ref, in_ref, up_out, down_out, split):
    device = Device(vel_ref[0])
    lane = iota(1)
    y, z = lane % 8, lane // 8
    source = jnp.where(device.ypos, y, 7 - y) * 16 + jnp.where(device.zpos, z, 15 - z)
    for plane in range(PLANES):
        for yhalf in (0, 1):
            split[plane, yhalf] = in_ref[plane, :, yhalf * LANES : (yhalf + 1) * LANES]
    for plane in range(PLANES):
        for yhalf in (0, 1):
            base = device.base(yhalf)
            for half, out in ((0, down_out), (1, up_out)):
                tiles = []
                for ix in range(CX):
                    rows = pl.ds(half * CX + ix, CZ, stride=2 * CX)
                    tiles.append(permuted(split[plane, yhalf, rows, :], source))
                for j, tile in enumerate(swapped(tiles)):
                    out[plane, base + j] = tile


def stream_kernel(vel_ref, up0, up1, up2, down0, down1, down2, up_out, down_out, mom_out, *scratch):
    first, second, sums = scratch
    device = Device(vel_ref[0])
    ay = time_step * jnp.abs(device.cy)
    az = time_step * jnp.abs(device.cz)

    for half in (0, 1):
        if half:
            field = [(up2, 0), (up2, 1)] + [(up1, p) for p in range(PLANES)]
            field += [(up0, p) for p in range(PLANES)]
            result = [(up_out, p) for p in range(PLANES)]
        else:
            field = [(down2, 1), (down2, 0)] + [(down1, p) for p in reversed(range(PLANES))]
            field += [(down0, p) for p in reversed(range(PLANES))]
            result = [(down_out, p) for p in reversed(range(PLANES))]
        ax = time_step * jnp.abs(cx_lanes(half))
        stages = [
            (field, [(first, p) for p in range(8)], 1.0 / 6.0, 0.0),
            ([(first, p) for p in range(8)], [(second, p) for p in range(6)], 1.0, 0.5),
            ([(second, p) for p in range(6)], result, 1.0, 1.0 / 3.0),
        ]
        for source, target, scale, part in stages:
            keep = scale * (1.0 - 1.5 * (ax + (ay + az)))
            x1, x2 = (2.0 * scale) * ax, (0.5 * scale) * ax
            y1, y2 = (2.0 * scale) * ay, (0.5 * scale) * ay
            z1, z2 = (2.0 * scale) * az, (0.5 * scale) * az
            for p, (out, plane) in enumerate(target):
                now = [source[p + 2][0][source[p + 2][1], y] for y in range(NY)]
                one, one_plane = source[p + 1]
                two, two_plane = source[p]
                start, start_plane = field[p + 10 - len(target)]
                for y in range(NY):
                    along_x = x1 * one[one_plane, y] - x2 * two[two_plane, y]
                    along_y = y1 * now[y - 1] - y2 * now[y - 2]
                    along_z = z1 * pltpu.roll(now[y], 8, 1) - z2 * pltpu.roll(now[y], 16, 1)
                    value = keep * now[y] + (along_x + (along_y + along_z))
                    if part:
                        value += part * start[start_plane, y]
                    out[plane, y] = value

    down_cx, up_cx = cx_lanes(0), cx_lanes(1)
    square = device.cy * device.cy + device.cz * device.cz
    down_square, up_square = square + down_cx * down_cx, square + up_cx * up_cx
    for plane in range(PLANES):
        for y in range(NY):
            down, up = down_out[plane, y], up_out[plane, y]
            both = down + up
            terms = (
                both,
                down_cx * down + up_cx * up,
                device.cz * both,
                down_square * down + up_square * up,
            )
            row = device.row(plane, y)
            for which, term in enumerate(terms):
                sums[which, pl.ds(row, 1), :] = jnp.sum(term, axis=0, keepdims=True)
    slot = iota(1) % 8
    for which, place in ((0, 0), (1, 1), (2, 3), (3, 4)):
        packed = jnp.zeros(TILE, jnp.float32)
        for j in range(8):
            tile = sums[which, 8 * j : 8 * j + 8, :]
            for w in (1, 2, 4):
                tile += pltpu.roll(tile, LANES - w, 1)
            packed = jnp.where(slot == j, pltpu.roll(tile, j, 1) if j else tile, packed)
        packed = weight * device.mirror_z(packed)
        mom_out[place] = packed
        if which == 0:
            mom_out[2] = device.cy * packed


def relax_kernel(last, vel_ref, mom_ref, up_in, down_in, *outs_and_scratch):
    *outs, rows, split = outs_and_scratch
    device = Device(vel_ref[0])
    rho = mom_ref[0]
    ux = mom_ref[1] / rho
    uy = mom_ref[2] / rho
    uz = mom_ref[3] / rho
    temp = (mom_ref[4] / rho - (ux * ux + uy * uy + uz * uz)) / 3.0
    minus_half = -0.5 / temp

    def factor(c, u, scale):
        return jnp.exp((c - u) * (c - u) * scale)

    def total(u):
        out = jnp.zeros_like(u)
        for i in range(NV1):
            out += factor(-speed_limit + spacing * i, u, minus_half)
        return out

    root = jnp.sqrt(temp)
    peak = rho / (temp * root)
    mass = weight * peak * total(ux) * total(uy) * total(uz)
    nu = time_step * rho * root / knudsen
    shrink = 1.0 / (1.0 + nu)
    common = nu * shrink * peak * (rho / mass) * factor(device.cy, uy, minus_half)

    slot = iota(1) % 8
    packed = [device.mirror_z(tile) for tile in (shrink, minus_half, uz, common, ux)]
    for j in range(8):
        spread = []
        for tile in packed:
            tile = jnp.where(slot == 0, pltpu.roll(tile, LANES - j, 1) if j else tile, 0.0)
            for w in (1, 2, 4):
                tile += pltpu.roll(tile, w, 1)
            spread.append(tile)
        keep, scale, drift_z, gain, drift_x = spread
        cells = slice(8 * j, 8 * j + 8)
        rows[0, cells, :] = keep
        rows[1, cells, :] = scale
        rows[2, cells, :] = drift_z
        for half in (0, 1):
            rows[3 + half, cells, :] = gain * factor(cx_lanes(half), drift_x, scale)

    lane = iota(1)
    y_lane, z_lane = lane // 16, lane % 16
    back = jnp.where(device.zpos, z_lane, 15 - z_lane) * 8 + jnp.where(device.ypos, y_lane, 7 - y_lane)
    for plane in range(PLANES):
        for yhalf in (0, 1):
            base = device.base(yhalf) if last else yhalf * 8
            values = ([], [])
            for j in range(8):
                y = base + j
                row = device.row(plane, y)
                keep, scale, drift_z, *gains = (
                    jnp.broadcast_to(rows[k, pl.ds(row, 1), :], TILE) for k in range(5)
                )
                along_z = factor(device.cz, drift_z, scale)
                for half, ref in ((0, down_in), (1, up_in)):
                    value = ref[plane, y] * keep + along_z * gains[half]
                    if last:
                        values[half].append(value)
                        continue
                    outs[half][plane, y] = value
                    if half == 0 and plane < 2:
                        outs[2][plane, y] = value
                    if half == 1 and plane >= 2:
                        outs[3][plane - 2, y] = value
            if last:
                for half in (0, 1):
                    for ix, tile in enumerate(swapped(values[half])):
                        where = pl.ds(half * CX + ix, CZ, stride=2 * CX)
                        split[plane, yhalf, where, :] = permuted(tile, back)
    if last:
        for plane in range(PLANES):
            for yhalf in (0, 1):
                outs[0][plane, :, yhalf * LANES : (yhalf + 1) * LANES] = split[plane, yhalf]


def vmem():
    return pl.BlockSpec(memory_space=pltpu.VMEM)


def smem():
    return pl.BlockSpec(memory_space=pltpu.SMEM)


def shape(*sizes):
    return jax.ShapeDtypeStruct(sizes, jnp.float32)


def call(body, name, out_shape, scratch, vel, *operands):
    return pl.pallas_call(
        body,
        in_specs=[smem()] + [vmem()] * len(operands),
        out_specs=[vmem()] * len(out_shape),
        out_shape=out_shape,
        scratch_shapes=[pltpu.VMEM(sizes, jnp.float32) for sizes in scratch],
        compiler_params=pltpu.CompilerParams(vmem_limit_bytes=8 << 20),
        name=name,
    )(vel, *operands)


def planes(count):
    return (count, NY, CZ, LANES)


def pack(vel, field):
    return call(pack_kernel, "pack", [shape(*planes(PLANES))] * 2, [SPLIT], vel, field)


def stream(vel, up, down):
    return call(
        stream_kernel,
        "stream",
        [shape(*planes(PLANES))] * 2 + [shape(5, *TILE)],
        [planes(8), planes(6), (4, ROWS, LANES)],
        vel,
        *up,
        *down,
    )


def relax(vel, moments, up, down, last):
    if last:
        out_shape = [shape(PLANES, COUNT, 2 * LANES)]
    else:
        out_shape = [shape(*planes(PLANES))] * 2 + [shape(*planes(2))] * 2

    def body(*refs):
        relax_kernel(last, *refs)

    name = "relax_last" if last else "relax"
    return call(body, name, out_shape, [(5, ROWS, LANES), SPLIT], vel, moments, up, down)


def passed_along(value, by):
    size = lax.axis_size("gx")
    return lax.ppermute(value, "gx", [(i, (i + by) % size) for i in range(size)])


def swapped_over(value, partner):
    size = lax.axis_size("vel")
    return lax.ppermute(value, "vel", [(i, partner(i)) for i in range(size)])


def summed_over_velocities(value):
    value = value + sum(swapped_over(value, lambda i, k=k: i ^ k) for k in (1, 2, 3))
    rounds = (
        lambda c: c ^ 1,
        lambda c: (c + 1) % 8 if c % 2 else (c - 1) % 8,
        lambda c: (3, 6, 5, 0, 7, 2, 1, 4)[c],
    )
    for chip in rounds:
        value = value + swapped_over(value, lambda i: 4 * chip(i // 4) + i % 4)
    return value


def on_device(distribution):
    vel = lax.axis_index("vel").astype(jnp.int32).reshape(1)
    up, down = pack(vel, distribution.transpose(1, 0, 2))
    up_far, down_far = up[2:], down[:2]
    for step in range(COLLISIONS):
        ups = (up, passed_along(up, 1), passed_along(up_far, 2))
        downs = (down, passed_along(down, -1), passed_along(down_far, -2))
        up_read, down_read, moments = stream(vel, ups, downs)
        moments = summed_over_velocities(moments)
        outs = relax(vel, moments, up_read, down_read, step == COLLISIONS - 1)
        if step < COLLISIONS - 1:
            down, up, down_far, up_far = outs
    return outs[0].transpose(1, 0, 2)


def solution(mesh):
    return jax.shard_map(
        on_device,
        mesh=mesh,
        in_specs=(P("vel", "gx", None),),
        out_specs=P("vel", "gx", None),
        check_vma=False,
    )
```

```python
import math

import jax
import jax.numpy as jnp
from jax import lax
from jax.experimental import pallas as pl
from jax.experimental.pallas import tpu as pltpu
from jax.sharding import PartitionSpec as P

NV1 = 16
COLLISIONS = 2

speed_limit = 4.0
time_step = 0.05
knudsen = 0.0125
spacing = 2.0 * speed_limit / (NV1 - 1)
weight = spacing**3 / (2.0 * math.pi) ** 1.5

PLANES = 4
NY = 16
CZ = 8
CX = 8
COUNT = 2 * CX * CZ
LANES = 128
TILE = (8, LANES)
ROWS = PLANES * NY
SPLIT = (PLANES, 2, COUNT, LANES)


def point(index):
    return -speed_limit + spacing * index.astype(jnp.float32)


def iota(dim):
    return lax.broadcasted_iota(jnp.int32, TILE, dim)


def cx_lanes(half):
    return point(half * CX + iota(1) % 8)


class Device:
    def __init__(self, vel):
        zhalf = vel % 2
        self.ypos = vel // 2 >= NV1 // 2
        self.zpos = zhalf == 1
        self.cy = point(vel // 2)
        self.cz = point(zhalf * CZ + iota(0))

    def row(self, plane, y):
        return plane * NY + jnp.where(self.ypos, y, NY - 1 - y)

    def base(self, yhalf):
        return jnp.where(self.ypos, yhalf, 1 - yhalf) * 8

    def mirror_z(self, tile):
        lane = iota(1)
        source = jnp.where(self.zpos, lane, (15 - lane // 8) * 8 + lane % 8)
        return permuted(tile, source)


def permuted(tile, source):
    return jnp.take_along_axis(tile, source, axis=1, mode="promise_in_bounds")


def swapped(tiles):
    tiles = list(tiles)
    lane = iota(1)
    for w in (1, 2, 4):
        high = (lane // w) % 2 == 1
        for i in range(8):
            if not i & w:
                a, b = tiles[i], tiles[i + w]
                tiles[i] = jnp.where(high, pltpu.roll(b, w, 1), a)
                tiles[i + w] = jnp.where(high, b, pltpu.roll(a, LANES - w, 1))
    return tiles


def pack_kernel(vel_ref, in_ref, up_out, down_out, split):
    device = Device(vel_ref[0])
    lane = iota(1)
    y, z = lane % 8, lane // 8
    source = jnp.where(device.ypos, y, 7 - y) * 16 + jnp.where(device.zpos, z, 15 - z)
    for plane in range(PLANES):
        for yhalf in (0, 1):
            split[plane, yhalf] = in_ref[plane, :, yhalf * LANES : (yhalf + 1) * LANES]
    for plane in range(PLANES):
        for yhalf in (0, 1):
            base = device.base(yhalf)
            for half, out in ((0, down_out), (1, up_out)):
                tiles = []
                for ix in range(CX):
                    rows = pl.ds(half * CX + ix, CZ, stride=2 * CX)
                    tiles.append(permuted(split[plane, yhalf, rows, :], source))
                for j, tile in enumerate(swapped(tiles)):
                    out[plane, base + j] = tile


def stream_kernel(vel_ref, up0, up1, up2, down0, down1, down2, up_out, down_out, mom_out, *scratch):
    first, second, sums = scratch
    device = Device(vel_ref[0])
    ay = time_step * jnp.abs(device.cy)
    az = time_step * jnp.abs(device.cz)

    for half in (0, 1):
        if half:
            field = [(up2, 0), (up2, 1)] + [(up1, p) for p in range(PLANES)]
            field += [(up0, p) for p in range(PLANES)]
            result = [(up_out, p) for p in range(PLANES)]
        else:
            field = [(down2, 1), (down2, 0)] + [(down1, p) for p in reversed(range(PLANES))]
            field += [(down0, p) for p in reversed(range(PLANES))]
            result = [(down_out, p) for p in reversed(range(PLANES))]
        ax = time_step * jnp.abs(cx_lanes(half))
        stages = [
            (field, [(first, p) for p in range(8)], 1.0 / 6.0, 0.0),
            ([(first, p) for p in range(8)], [(second, p) for p in range(6)], 1.0, 0.5),
            ([(second, p) for p in range(6)], result, 1.0, 1.0 / 3.0),
        ]
        for source, target, scale, part in stages:
            keep = scale * (1.0 - 1.5 * (ax + (ay + az)))
            x1, x2 = (2.0 * scale) * ax, (0.5 * scale) * ax
            y1, y2 = (2.0 * scale) * ay, (0.5 * scale) * ay
            z1, z2 = (2.0 * scale) * az, (0.5 * scale) * az
            for p, (out, plane) in enumerate(target):
                now = [source[p + 2][0][source[p + 2][1], y] for y in range(NY)]
                one, one_plane = source[p + 1]
                two, two_plane = source[p]
                start, start_plane = field[p + 10 - len(target)]
                for y in range(NY):
                    along_x = x1 * one[one_plane, y] - x2 * two[two_plane, y]
                    along_y = y1 * now[y - 1] - y2 * now[y - 2]
                    along_z = z1 * pltpu.roll(now[y], 8, 1) - z2 * pltpu.roll(now[y], 16, 1)
                    value = keep * now[y] + (along_x + (along_y + along_z))
                    if part:
                        value += part * start[start_plane, y]
                    out[plane, y] = value

    down_cx, up_cx = cx_lanes(0), cx_lanes(1)
    square = device.cy * device.cy + device.cz * device.cz
    down_square, up_square = square + down_cx * down_cx, square + up_cx * up_cx
    for plane in range(PLANES):
        for y in range(NY):
            down, up = down_out[plane, y], up_out[plane, y]
            both = down + up
            terms = (
                both,
                down_cx * down + up_cx * up,
                device.cz * both,
                down_square * down + up_square * up,
            )
            row = device.row(plane, y)
            for which, term in enumerate(terms):
                sums[which, pl.ds(row, 1), :] = jnp.sum(term, axis=0, keepdims=True)
    slot = iota(1) % 8
    for which, place in ((0, 0), (1, 1), (2, 3), (3, 4)):
        packed = jnp.zeros(TILE, jnp.float32)
        for j in range(8):
            tile = sums[which, 8 * j : 8 * j + 8, :]
            for w in (1, 2, 4):
                tile += pltpu.roll(tile, LANES - w, 1)
            packed = jnp.where(slot == j, pltpu.roll(tile, j, 1) if j else tile, packed)
        packed = weight * device.mirror_z(packed)
        mom_out[place] = packed
        if which == 0:
            mom_out[2] = device.cy * packed


def relax_kernel(last, vel_ref, mom_ref, up_in, down_in, *outs_and_scratch):
    *outs, rows, split = outs_and_scratch
    device = Device(vel_ref[0])
    rho = mom_ref[0]
    ux = mom_ref[1] / rho
    uy = mom_ref[2] / rho
    uz = mom_ref[3] / rho
    temp = (mom_ref[4] / rho - (ux * ux + uy * uy + uz * uz)) / 3.0
    minus_half = -0.5 / temp

    def factor(c, u, scale):
        return jnp.exp((c - u) * (c - u) * scale)

    def total(u):
        out = jnp.zeros_like(u)
        for i in range(NV1):
            out += factor(-speed_limit + spacing * i, u, minus_half)
        return out

    root = jnp.sqrt(temp)
    peak = rho / (temp * root)
    mass = weight * peak * total(ux) * total(uy) * total(uz)
    nu = time_step * rho * root / knudsen
    shrink = 1.0 / (1.0 + nu)
    common = nu * shrink * peak * (rho / mass) * factor(device.cy, uy, minus_half)

    slot = iota(1) % 8
    packed = [device.mirror_z(tile) for tile in (shrink, minus_half, uz, common, ux)]
    for j in range(8):
        spread = []
        for tile in packed:
            tile = jnp.where(slot == 0, pltpu.roll(tile, LANES - j, 1) if j else tile, 0.0)
            for w in (1, 2, 4):
                tile += pltpu.roll(tile, w, 1)
            spread.append(tile)
        keep, scale, drift_z, gain, drift_x = spread
        cells = slice(8 * j, 8 * j + 8)
        rows[0, cells, :] = keep
        rows[1, cells, :] = scale
        rows[2, cells, :] = drift_z
        for half in (0, 1):
            rows[3 + half, cells, :] = gain * factor(cx_lanes(half), drift_x, scale)

    lane = iota(1)
    y_lane, z_lane = lane // 16, lane % 16
    back = jnp.where(device.zpos, z_lane, 15 - z_lane) * 8 + jnp.where(device.ypos, y_lane, 7 - y_lane)
    for plane in range(PLANES):
        for yhalf in (0, 1):
            base = device.base(yhalf) if last else yhalf * 8
            values = ([], [])
            for j in range(8):
                y = base + j
                row = device.row(plane, y)
                keep, scale, drift_z, *gains = (
                    jnp.broadcast_to(rows[k, pl.ds(row, 1), :], TILE) for k in range(5)
                )
                along_z = factor(device.cz, drift_z, scale)
                for half, ref in ((0, down_in), (1, up_in)):
                    value = ref[plane, y] * keep + along_z * gains[half]
                    if last:
                        values[half].append(value)
                        continue
                    outs[half][plane, y] = value
                    if half == 0 and plane < 2:
                        outs[2][plane, y] = value
                    if half == 1 and plane >= 2:
                        outs[3][plane - 2, y] = value
            if last:
                for half in (0, 1):
                    for ix, tile in enumerate(swapped(values[half])):
                        where = pl.ds(half * CX + ix, CZ, stride=2 * CX)
                        split[plane, yhalf, where, :] = permuted(tile, back)
    if last:
        for plane in range(PLANES):
            for yhalf in (0, 1):
                outs[0][plane, :, yhalf * LANES : (yhalf + 1) * LANES] = split[plane, yhalf]


def vmem():
    return pl.BlockSpec(memory_space=pltpu.VMEM)


def smem():
    return pl.BlockSpec(memory_space=pltpu.SMEM)


def shape(*sizes):
    return jax.ShapeDtypeStruct(sizes, jnp.float32)


def call(body, name, out_shape, scratch, vel, *operands):
    return pl.pallas_call(
        body,
        in_specs=[smem()] + [vmem()] * len(operands),
        out_specs=[vmem()] * len(out_shape),
        out_shape=out_shape,
        scratch_shapes=[pltpu.VMEM(sizes, jnp.float32) for sizes in scratch],
        compiler_params=pltpu.CompilerParams(vmem_limit_bytes=8 << 20),
        name=name,
    )(vel, *operands)


def planes(count):
    return (count, NY, CZ, LANES)


def pack(vel, field):
    return call(pack_kernel, "pack", [shape(*planes(PLANES))] * 2, [SPLIT], vel, field)


def stream(vel, up, down):
    return call(
        stream_kernel,
        "stream",
        [shape(*planes(PLANES))] * 2 + [shape(5, *TILE)],
        [planes(8), planes(6), (4, ROWS, LANES)],
        vel,
        *up,
        *down,
    )


def relax(vel, moments, up, down, last):
    if last:
        out_shape = [shape(PLANES, COUNT, 2 * LANES)]
    else:
        out_shape = [shape(*planes(PLANES))] * 2 + [shape(*planes(2))] * 2

    def body(*refs):
        relax_kernel(last, *refs)

    name = "relax_last" if last else "relax"
    return call(body, name, out_shape, [(5, ROWS, LANES), SPLIT], vel, moments, up, down)


def passed_along(value, by):
    size = lax.axis_size("gx")
    return lax.ppermute(value, "gx", [(i, (i + by) % size) for i in range(size)])


def swapped_over(value, partner):
    size = lax.axis_size("vel")
    return lax.ppermute(value, "vel", [(i, partner(i)) for i in range(size)])


def summed_over_velocities(value):
    for step in (1, 4):
        value = value + sum(swapped_over(value, lambda i, k=k: i ^ (step * k)) for k in (1, 2, 3))
    return value + swapped_over(value, lambda i: 4 * (7 - i // 4) + i % 4)


def on_device(distribution):
    vel = lax.axis_index("vel").astype(jnp.int32).reshape(1)
    up, down = pack(vel, distribution.transpose(1, 0, 2))
    up_far, down_far = up[2:], down[:2]
    for step in range(COLLISIONS):
        ups = (up, passed_along(up, 1), passed_along(up_far, 2))
        downs = (down, passed_along(down, -1), passed_along(down_far, -2))
        up_read, down_read, moments = stream(vel, ups, downs)
        moments = summed_over_velocities(moments)
        outs = relax(vel, moments, up_read, down_read, step == COLLISIONS - 1)
        if step < COLLISIONS - 1:
            down, up, down_far, up_far = outs
    return outs[0].transpose(1, 0, 2)


def solution(mesh):
    return jax.shard_map(
        on_device,
        mesh=mesh,
        in_specs=(P("vel", "gx", None),),
        out_specs=P("vel", "gx", None),
        check_vma=False,
    )
```

```python
import math

import jax
import jax.numpy as jnp
from jax import lax
from jax.experimental import pallas as pl
from jax.experimental.pallas import tpu as pltpu
from jax.sharding import PartitionSpec as P

NV1 = 16
COLLISIONS = 2

speed_limit = 4.0
time_step = 0.05
knudsen = 0.0125
spacing = 2.0 * speed_limit / (NV1 - 1)
weight = spacing**3 / (2.0 * math.pi) ** 1.5

PLANES = 4
NY = 16
CZ = 8
CX = 8
COUNT = 2 * CX * CZ
LANES = 128
TILE = (8, LANES)
ROWS = PLANES * NY


def point(index):
    return -speed_limit + spacing * index.astype(jnp.float32)


def iota(dim):
    return lax.broadcasted_iota(jnp.int32, TILE, dim)


def cx_lanes(half):
    return point(half * CX + iota(1) % 8)


class Device:
    def __init__(self, vel):
        zhalf = vel % 2
        self.ypos = vel // 2 >= NV1 // 2
        self.zpos = zhalf == 1
        self.cy = point(vel // 2)
        self.cz = point(zhalf * CZ + iota(0))

    def row(self, plane, y):
        return plane * NY + jnp.where(self.ypos, y, NY - 1 - y)

    def base(self, yhalf):
        return jnp.where(self.ypos, yhalf, 1 - yhalf) * 8

    def mirror_z(self, tile):
        lane = iota(1)
        source = jnp.where(self.zpos, lane, (15 - lane // 8) * 8 + lane % 8)
        return permuted(tile, source)


def permuted(tile, source):
    return jnp.take_along_axis(tile, source, axis=1, mode="promise_in_bounds")


def swapped(tiles):
    tiles = list(tiles)
    lane = iota(1)
    for w in (1, 2, 4):
        high = (lane // w) % 2 == 1
        for i in range(8):
            if not i & w:
                a, b = tiles[i], tiles[i + w]
                tiles[i] = jnp.where(high, pltpu.roll(b, w, 1), a)
                tiles[i + w] = jnp.where(high, b, pltpu.roll(a, LANES - w, 1))
    return tiles


def native_rows(half, ix, plane, yhalf):
    return pl.ds((half * CX + ix) * 8 + yhalf * 4 + plane, CZ, stride=2 * CX * 8)


def pack_kernel(half, vel_ref, in_ref, out):
    device = Device(vel_ref[0])
    lane = iota(1)
    y, z = lane % 8, lane // 8
    source = jnp.where(device.ypos, y, 7 - y) * 16 + jnp.where(device.zpos, z, 15 - z)
    for plane in range(PLANES):
        for yhalf in (0, 1):
            base = device.base(yhalf)
            tiles = [
                permuted(in_ref[native_rows(half, ix, plane, yhalf), :], source)
                for ix in range(CX)
            ]
            for j, tile in enumerate(swapped(tiles)):
                out[plane, base + j] = tile


def stream_kernel(vel_ref, up0, up1, up2, down0, down1, down2, up_out, down_out, mom_out, *scratch):
    first, second, sums = scratch
    device = Device(vel_ref[0])
    ay = time_step * jnp.abs(device.cy)
    az = time_step * jnp.abs(device.cz)

    for half in (0, 1):
        if half:
            field = [(up2, 0), (up2, 1)] + [(up1, p) for p in range(PLANES)]
            field += [(up0, p) for p in range(PLANES)]
            result = [(up_out, p) for p in range(PLANES)]
        else:
            field = [(down2, 1), (down2, 0)] + [(down1, p) for p in reversed(range(PLANES))]
            field += [(down0, p) for p in reversed(range(PLANES))]
            result = [(down_out, p) for p in reversed(range(PLANES))]
        ax = time_step * jnp.abs(cx_lanes(half))
        stages = [
            (field, [(first, p) for p in range(8)], 1.0 / 6.0, 0.0),
            ([(first, p) for p in range(8)], [(second, p) for p in range(6)], 1.0, 0.5),
            ([(second, p) for p in range(6)], result, 1.0, 1.0 / 3.0),
        ]
        for source, target, scale, part in stages:
            keep = scale * (1.0 - 1.5 * (ax + (ay + az)))
            x1, x2 = (2.0 * scale) * ax, (0.5 * scale) * ax
            y1, y2 = (2.0 * scale) * ay, (0.5 * scale) * ay
            z1, z2 = (2.0 * scale) * az, (0.5 * scale) * az
            for p, (out, plane) in enumerate(target):
                now = [source[p + 2][0][source[p + 2][1], y] for y in range(NY)]
                one, one_plane = source[p + 1]
                two, two_plane = source[p]
                start, start_plane = field[p + 10 - len(target)]
                for y in range(NY):
                    along_x = x1 * one[one_plane, y] - x2 * two[two_plane, y]
                    along_y = y1 * now[y - 1] - y2 * now[y - 2]
                    along_z = z1 * pltpu.roll(now[y], 8, 1) - z2 * pltpu.roll(now[y], 16, 1)
                    value = keep * now[y] + (along_x + (along_y + along_z))
                    if part:
                        value += part * start[start_plane, y]
                    out[plane, y] = value

    down_cx, up_cx = cx_lanes(0), cx_lanes(1)
    square = device.cy * device.cy + device.cz * device.cz
    down_square, up_square = square + down_cx * down_cx, square + up_cx * up_cx
    for plane in range(PLANES):
        for y in range(NY):
            down, up = down_out[plane, y], up_out[plane, y]
            both = down + up
            terms = (
                both,
                down_cx * down + up_cx * up,
                device.cz * both,
                down_square * down + up_square * up,
            )
            row = device.row(plane, y)
            for which, term in enumerate(terms):
                sums[which, pl.ds(row, 1), :] = jnp.sum(term, axis=0, keepdims=True)
    slot = iota(1) % 8
    for which, place in ((0, 0), (1, 1), (2, 3), (3, 4)):
        packed = jnp.zeros(TILE, jnp.float32)
        for j in range(8):
            tile = sums[which, 8 * j : 8 * j + 8, :]
            for w in (1, 2, 4):
                tile += pltpu.roll(tile, LANES - w, 1)
            packed = jnp.where(slot == j, pltpu.roll(tile, j, 1) if j else tile, packed)
        packed = weight * device.mirror_z(packed)
        mom_out[place] = packed
        if which == 0:
            mom_out[2] = device.cy * packed


def relax_kernel(last, vel_ref, mom_ref, up_in, down_in, *outs_and_scratch):
    *outs, rows = outs_and_scratch
    device = Device(vel_ref[0])
    rho = mom_ref[0]
    ux = mom_ref[1] / rho
    uy = mom_ref[2] / rho
    uz = mom_ref[3] / rho
    temp = (mom_ref[4] / rho - (ux * ux + uy * uy + uz * uz)) / 3.0
    minus_half = -0.5 / temp

    def factor(c, u, scale):
        return jnp.exp((c - u) * (c - u) * scale)

    def total(u):
        out = jnp.zeros_like(u)
        for i in range(NV1):
            out += factor(-speed_limit + spacing * i, u, minus_half)
        return out

    root = jnp.sqrt(temp)
    peak = rho / (temp * root)
    mass = weight * peak * total(ux) * total(uy) * total(uz)
    nu = time_step * rho * root / knudsen
    shrink = 1.0 / (1.0 + nu)
    common = nu * shrink * peak * (rho / mass) * factor(device.cy, uy, minus_half)

    slot = iota(1) % 8
    packed = [device.mirror_z(tile) for tile in (shrink, minus_half, uz, common, ux)]
    for j in range(8):
        spread = []
        for tile in packed:
            tile = jnp.where(slot == 0, pltpu.roll(tile, LANES - j, 1) if j else tile, 0.0)
            for w in (1, 2, 4):
                tile += pltpu.roll(tile, w, 1)
            spread.append(tile)
        keep, scale, drift_z, gain, drift_x = spread
        cells = slice(8 * j, 8 * j + 8)
        rows[0, cells, :] = keep
        rows[1, cells, :] = scale
        rows[2, cells, :] = drift_z
        for half in (0, 1):
            rows[3 + half, cells, :] = gain * factor(cx_lanes(half), drift_x, scale)

    lane = iota(1)
    y_lane, z_lane = lane // 16, lane % 16
    back = jnp.where(device.zpos, z_lane, 15 - z_lane) * 8 + jnp.where(device.ypos, y_lane, 7 - y_lane)
    for plane in range(PLANES):
        for yhalf in (0, 1):
            base = device.base(yhalf) if last else yhalf * 8
            values = ([], [])
            for j in range(8):
                y = base + j
                row = device.row(plane, y)
                keep, scale, drift_z, *gains = (
                    jnp.broadcast_to(rows[k, pl.ds(row, 1), :], TILE) for k in range(5)
                )
                along_z = factor(device.cz, drift_z, scale)
                for half, ref in ((0, down_in), (1, up_in)):
                    value = ref[plane, y] * keep + along_z * gains[half]
                    if last:
                        values[half].append(value)
                        continue
                    outs[half][plane, y] = value
                    if half == 0 and plane < 2:
                        outs[2][plane, y] = value
                    if half == 1 and plane >= 2:
                        outs[3][plane - 2, y] = value
            if last:
                for half in (0, 1):
                    for ix, tile in enumerate(swapped(values[half])):
                        outs[0][native_rows(half, ix, plane, yhalf), :] = permuted(tile, back)


def vmem():
    return pl.BlockSpec(memory_space=pltpu.VMEM)


def smem():
    return pl.BlockSpec(memory_space=pltpu.SMEM)


def shape(*sizes):
    return jax.ShapeDtypeStruct(sizes, jnp.float32)


def call(body, name, out_shape, scratch, vel, *operands):
    return pl.pallas_call(
        body,
        in_specs=[smem()] + [vmem()] * len(operands),
        out_specs=[vmem()] * len(out_shape),
        out_shape=out_shape,
        scratch_shapes=[pltpu.VMEM(sizes, jnp.float32) for sizes in scratch],
        compiler_params=pltpu.CompilerParams(vmem_limit_bytes=8 << 20),
        name=name,
    )(vel, *operands)


def planes(count):
    return (count, NY, CZ, LANES)


def pack(vel, field, half):
    def body(*refs):
        pack_kernel(half, *refs)

    name = "pack_up" if half else "pack_down"
    return call(body, name, [shape(*planes(PLANES))], [], vel, field)[0]


def stream(vel, up, down):
    return call(
        stream_kernel,
        "stream",
        [shape(*planes(PLANES))] * 2 + [shape(5, *TILE)],
        [planes(8), planes(6), (4, ROWS, LANES)],
        vel,
        *up,
        *down,
    )


def relax(vel, moments, up, down, last):
    if last:
        out_shape = [shape(8 * COUNT, LANES)]
    else:
        out_shape = [shape(*planes(PLANES))] * 2 + [shape(*planes(2))] * 2

    def body(*refs):
        relax_kernel(last, *refs)

    name = "relax_last" if last else "relax"
    return call(body, name, out_shape, [(5, ROWS, LANES)], vel, moments, up, down)


def passed_along(value, by):
    size = lax.axis_size("gx")
    return lax.ppermute(value, "gx", [(i, (i + by) % size) for i in range(size)])


def swapped_over(value, partner):
    size = lax.axis_size("vel")
    return lax.ppermute(value, "vel", [(i, partner(i)) for i in range(size)])


def summed_over_velocities(value):
    for step in (1, 4):
        value = value + sum(swapped_over(value, lambda i, k=k: i ^ (step * k)) for k in (1, 2, 3))
    return value + swapped_over(value, lambda i: 4 * (7 - i // 4) + i % 4)


def on_device(distribution):
    vel = lax.axis_index("vel").astype(jnp.int32).reshape(1)
    field = distribution.reshape(COUNT, PLANES, 2, LANES).transpose(0, 2, 1, 3)
    field = field.reshape(8 * COUNT, LANES)
    up, down = pack(vel, field, 1), pack(vel, field, 0)
    up_far, down_far = up[2:], down[:2]
    for step in range(COLLISIONS):
        ups = (up, passed_along(up, 1), passed_along(up_far, 2))
        downs = (down, passed_along(down, -1), passed_along(down_far, -2))
        up_read, down_read, moments = stream(vel, ups, downs)
        moments = summed_over_velocities(moments)
        outs = relax(vel, moments, up_read, down_read, step == COLLISIONS - 1)
        if step < COLLISIONS - 1:
            down, up, down_far, up_far = outs
    field = outs[0].reshape(COUNT, 2, PLANES, LANES).transpose(0, 2, 1, 3)
    return field.reshape(distribution.shape)


def solution(mesh):
    return jax.shard_map(
        on_device,
        mesh=mesh,
        in_specs=(P("vel", "gx", None),),
        out_specs=P("vel", "gx", None),
        check_vma=False,
    )
```

```python
import math

import jax
import jax.numpy as jnp
from jax import lax
from jax.experimental import pallas as pl
from jax.experimental.pallas import tpu as pltpu
from jax.sharding import PartitionSpec as P

NV1 = 16
COLLISIONS = 2

speed_limit = 4.0
time_step = 0.05
knudsen = 0.0125
spacing = 2.0 * speed_limit / (NV1 - 1)
weight = spacing**3 / (2.0 * math.pi) ** 1.5

PLANES = 4
NY = 16
CZ = 8
CX = 8
COUNT = 2 * CX * CZ
LANES = 128
TILE = (8, LANES)
ROWS = PLANES * NY


def point(index):
    return -speed_limit + spacing * index.astype(jnp.float32)


def iota(dim):
    return lax.broadcasted_iota(jnp.int32, TILE, dim)


def cx_lanes(half):
    return point(half * CX + iota(1) % 8)


class Device:
    def __init__(self, vel):
        zhalf = vel % 2
        self.ypos = vel // 2 >= NV1 // 2
        self.zpos = zhalf == 1
        self.cy = point(vel // 2)
        self.cz = point(zhalf * CZ + iota(0))

    def row(self, plane, y):
        return plane * NY + jnp.where(self.ypos, y, NY - 1 - y)

    def base(self, yhalf):
        return jnp.where(self.ypos, yhalf, 1 - yhalf) * 8

    def mirror_z(self, tile):
        lane = iota(1)
        source = jnp.where(self.zpos, lane, (15 - lane // 8) * 8 + lane % 8)
        return permuted(tile, source)


def permuted(tile, source):
    return jnp.take_along_axis(tile, source, axis=1, mode="promise_in_bounds")


def swapped(tiles):
    tiles = list(tiles)
    lane = iota(1)
    for w in (1, 2, 4):
        high = (lane // w) % 2 == 1
        for i in range(8):
            if not i & w:
                a, b = tiles[i], tiles[i + w]
                tiles[i] = jnp.where(high, pltpu.roll(b, w, 1), a)
                tiles[i + w] = jnp.where(high, b, pltpu.roll(a, LANES - w, 1))
    return tiles


def native_rows(half, ix, plane, yhalf):
    return pl.ds((half * CX + ix) * 8 + yhalf * 4 + plane, CZ, stride=2 * CX * 8)


def pack_kernel(half, vel_ref, in_ref, out):
    device = Device(vel_ref[0])
    lane = iota(1)
    y, z = lane % 8, lane // 8
    source = jnp.where(device.ypos, y, 7 - y) * 16 + jnp.where(device.zpos, z, 15 - z)
    for plane in range(PLANES):
        for yhalf in (0, 1):
            base = device.base(yhalf)
            tiles = [
                permuted(in_ref[native_rows(half, ix, plane, yhalf), :], source)
                for ix in range(CX)
            ]
            for j, tile in enumerate(swapped(tiles)):
                out[plane, base + j] = tile


def stream_kernel(vel_ref, up0, up1, up2, down0, down1, down2, up_out, down_out, mom_out, *scratch):
    first, second, sums = scratch
    device = Device(vel_ref[0])
    ay = time_step * jnp.abs(device.cy)
    az = time_step * jnp.abs(device.cz)

    for half in (0, 1):
        if half:
            field = [(up2, 0), (up2, 1)] + [(up1, p) for p in range(PLANES)]
            field += [(up0, p) for p in range(PLANES)]
            result = [(up_out, p) for p in range(PLANES)]
        else:
            field = [(down2, 1), (down2, 0)] + [(down1, p) for p in reversed(range(PLANES))]
            field += [(down0, p) for p in reversed(range(PLANES))]
            result = [(down_out, p) for p in reversed(range(PLANES))]
        ax = time_step * jnp.abs(cx_lanes(half))
        stages = [
            (field, [(first, p) for p in range(8)], 1.0 / 6.0, 0.0),
            ([(first, p) for p in range(8)], [(second, p) for p in range(6)], 1.0, 0.5),
            ([(second, p) for p in range(6)], result, 1.0, 1.0 / 3.0),
        ]
        for source, target, scale, part in stages:
            keep = scale * (1.0 - 1.5 * (ax + (ay + az)))
            x1, x2 = (2.0 * scale) * ax, (0.5 * scale) * ax
            y1, y2 = (2.0 * scale) * ay, (0.5 * scale) * ay
            z1, z2 = (2.0 * scale) * az, (0.5 * scale) * az
            for p, (out, plane) in enumerate(target):
                now = [source[p + 2][0][source[p + 2][1], y] for y in range(NY)]
                one, one_plane = source[p + 1]
                two, two_plane = source[p]
                start, start_plane = field[p + 10 - len(target)]
                for y in range(NY):
                    along_x = x1 * one[one_plane, y] - x2 * two[two_plane, y]
                    along_y = y1 * now[y - 1] - y2 * now[y - 2]
                    along_z = z1 * pltpu.roll(now[y], 8, 1) - z2 * pltpu.roll(now[y], 16, 1)
                    value = keep * now[y] + (along_x + (along_y + along_z))
                    if part:
                        value += part * start[start_plane, y]
                    out[plane, y] = value

    down_cx, up_cx = cx_lanes(0), cx_lanes(1)
    square = device.cy * device.cy + device.cz * device.cz
    down_square, up_square = square + down_cx * down_cx, square + up_cx * up_cx
    for plane in range(PLANES):
        for y in range(NY):
            down, up = down_out[plane, y], up_out[plane, y]
            both = down + up
            terms = (
                both,
                down_cx * down + up_cx * up,
                device.cz * both,
                down_square * down + up_square * up,
            )
            row = device.row(plane, y)
            for which, term in enumerate(terms):
                sums[which, pl.ds(row, 1), :] = jnp.sum(term, axis=0, keepdims=True)
    slot = iota(1) % 8
    for which, place in ((0, 0), (1, 1), (2, 3), (3, 4)):
        packed = jnp.zeros(TILE, jnp.float32)
        for j in range(8):
            tile = sums[which, 8 * j : 8 * j + 8, :]
            for w in (1, 2, 4):
                tile += pltpu.roll(tile, LANES - w, 1)
            packed = jnp.where(slot == j, pltpu.roll(tile, j, 1) if j else tile, packed)
        packed = weight * device.mirror_z(packed)
        mom_out[place] = packed
        if which == 0:
            mom_out[2] = device.cy * packed


def relax_kernel(last, vel_ref, mom_ref, up_in, down_in, *outs_and_scratch):
    *outs, rows = outs_and_scratch
    device = Device(vel_ref[0])
    rho = mom_ref[0]
    ux = mom_ref[1] / rho
    uy = mom_ref[2] / rho
    uz = mom_ref[3] / rho
    temp = (mom_ref[4] / rho - (ux * ux + uy * uy + uz * uz)) / 3.0
    minus_half = -0.5 / temp

    def factor(c, u, scale):
        return jnp.exp((c - u) * (c - u) * scale)

    def total(u):
        out = jnp.zeros_like(u)
        for i in range(NV1):
            out += factor(-speed_limit + spacing * i, u, minus_half)
        return out

    root = jnp.sqrt(temp)
    peak = rho / (temp * root)
    mass = weight * peak * total(ux) * total(uy) * total(uz)
    nu = time_step * rho * root / knudsen
    shrink = 1.0 / (1.0 + nu)
    common = nu * shrink * peak * (rho / mass) * factor(device.cy, uy, minus_half)

    slot = iota(1) % 8
    packed = [device.mirror_z(tile) for tile in (shrink, minus_half, uz, common, ux)]
    for j in range(8):
        spread = []
        for tile in packed:
            tile = jnp.where(slot == 0, pltpu.roll(tile, LANES - j, 1) if j else tile, 0.0)
            for w in (1, 2, 4):
                tile += pltpu.roll(tile, w, 1)
            spread.append(tile)
        keep, scale, drift_z, gain, drift_x = spread
        cells = slice(8 * j, 8 * j + 8)
        rows[0, cells, :] = keep
        rows[1, cells, :] = scale
        rows[2, cells, :] = drift_z
        for half in (0, 1):
            rows[3 + half, cells, :] = gain * factor(cx_lanes(half), drift_x, scale)

    lane = iota(1)
    y_lane, z_lane = lane // 16, lane % 16
    back = jnp.where(device.zpos, z_lane, 15 - z_lane) * 8 + jnp.where(device.ypos, y_lane, 7 - y_lane)
    for plane in range(PLANES):
        for yhalf in (0, 1):
            base = device.base(yhalf) if last else yhalf * 8
            values = ([], [])
            for j in range(8):
                y = base + j
                row = device.row(plane, y)
                keep, scale, drift_z, *gains = (
                    jnp.broadcast_to(rows[k, pl.ds(row, 1), :], TILE) for k in range(5)
                )
                along_z = factor(device.cz, drift_z, scale)
                for half, ref in ((0, down_in), (1, up_in)):
                    value = ref[plane, y] * keep + along_z * gains[half]
                    if last:
                        values[half].append(value)
                        continue
                    outs[half][plane, y] = value
                    if half == 0 and plane < 2:
                        outs[2][plane, y] = value
                    if half == 1 and plane >= 2:
                        outs[3][plane - 2, y] = value
            if last:
                for half in (0, 1):
                    for ix, tile in enumerate(swapped(values[half])):
                        outs[0][native_rows(half, ix, plane, yhalf), :] = permuted(tile, back)


def vmem():
    return pl.BlockSpec(memory_space=pltpu.VMEM)


def smem():
    return pl.BlockSpec(memory_space=pltpu.SMEM)


def shape(*sizes):
    return jax.ShapeDtypeStruct(sizes, jnp.float32)


def call(body, name, out_shape, scratch, vel, *operands):
    return pl.pallas_call(
        body,
        in_specs=[smem()] + [vmem()] * len(operands),
        out_specs=[vmem()] * len(out_shape),
        out_shape=out_shape,
        scratch_shapes=[pltpu.VMEM(sizes, jnp.float32) for sizes in scratch],
        compiler_params=pltpu.CompilerParams(vmem_limit_bytes=8 << 20),
        name=name,
    )(vel, *operands)


def planes(count):
    return (count, NY, CZ, LANES)


def pack(vel, field, half):
    def body(*refs):
        pack_kernel(half, *refs)

    name = "pack_up" if half else "pack_down"
    return call(body, name, [shape(*planes(PLANES))], [], vel, field)[0]


def stream(vel, up, down):
    return call(
        stream_kernel,
        "stream",
        [shape(*planes(PLANES))] * 2 + [shape(5, *TILE)],
        [planes(8), planes(6), (4, ROWS, LANES)],
        vel,
        *up,
        *down,
    )


def relax(vel, moments, up, down, last):
    if last:
        out_shape = [shape(8 * COUNT, LANES)]
    else:
        out_shape = [shape(*planes(PLANES))] * 2 + [shape(*planes(2))] * 2

    def body(*refs):
        relax_kernel(last, *refs)

    name = "relax_last" if last else "relax"
    return call(body, name, out_shape, [(5, ROWS, LANES)], vel, moments, up, down)


def passed_along(value, by):
    size = lax.axis_size("gx")
    return lax.ppermute(value, "gx", [(i, (i + by) % size) for i in range(size)])


def swapped_over(value, partner):
    size = lax.axis_size("vel")
    return lax.ppermute(value, "vel", [(i, partner(i)) for i in range(size)])


def summed_over_velocities(value):
    for step in (4, 1):
        value = value + sum(swapped_over(value, lambda i, k=k: i ^ (step * k)) for k in (1, 2, 3))
    return value + swapped_over(value, lambda i: 4 * (7 - i // 4) + i % 4)


def on_device(distribution):
    vel = lax.axis_index("vel").astype(jnp.int32).reshape(1)
    field = distribution.reshape(COUNT, PLANES, 2, LANES).transpose(0, 2, 1, 3)
    field = field.reshape(8 * COUNT, LANES)
    up, down = pack(vel, field, 1), pack(vel, field, 0)
    up_far, down_far = up[2:], down[:2]
    for step in range(COLLISIONS):
        ups = (up, passed_along(up, 1), passed_along(up_far, 2))
        downs = (down, passed_along(down, -1), passed_along(down_far, -2))
        up_read, down_read, moments = stream(vel, ups, downs)
        moments = summed_over_velocities(moments)
        outs = relax(vel, moments, up_read, down_read, step == COLLISIONS - 1)
        if step < COLLISIONS - 1:
            down, up, down_far, up_far = outs
    field = outs[0].reshape(COUNT, 2, PLANES, LANES).transpose(0, 2, 1, 3)
    return field.reshape(distribution.shape)


def solution(mesh):
    return jax.shard_map(
        on_device,
        mesh=mesh,
        in_specs=(P("vel", "gx", None),),
        out_specs=P("vel", "gx", None),
        check_vma=False,
    )
```
